256 devices in a mesh: sx: 16 (over y, z_lo), sy: 16 (over z_hi, x, core).
Axes of the slice: x: 4, y: 4, z: 8 (z_hi: 2, z_lo: 4; z = z_hi * 4 + z_lo), core: 2. Of those that a mesh axis runs over, the one named last changes fastest.
Arguments:
- schur: float32 [16, 16, 1024, 1024], P('sx', 'sy'), may hold values from -60 to 300, as said below
- rhs_local: float32 [16, 16, 1024], P('sx', 'sy'), may hold values from -1 to 10
- edge_perm: int32 [16, 16, 4, 2], P('sx', 'sy'), may hold values from 0 to 1, each once within a row
- chol_interior: float32 [16, 16, 512, 512], P('sx', 'sy'), may hold values from -1 to 2, as said below
- coupling: bfloat16 [16, 16, 512, 1024], P('sx', 'sy'), may hold values from -0.25 to 0.25
- boundary_diag: float32 [16, 16, 1024], P('sx', 'sy'), may hold values from 1 to 3
- restrict: bfloat16 [16, 16, 768, 1024], P('sx', 'sy'), may hold values from -0.1875 to 0.1875
- extend: bfloat16 [16, 16, 1024, 768], P('sx', 'sy'), may hold values from -0.1875 to 0.1875
Outputs:
- solution: float32 [16, 16, 1024], P('sx', 'sy')
- residual: float32 [16, 16, 1024], P('sx', 'sy')
- schur_next: bfloat16 [16, 16, 1024, 1024], P('sx', 'sy')
- coarse: float32 [768, 768], P('sx', 'sy')
The draws below stay inside these ranges and needn't reach their ends.
Inputs may be any that keep to these rules, and one draw needn't show every extreme that they name: `schur`: each subdomain's matrix is symmetric positive definite; its scale differs from subdomain to subdomain. `chol_interior`: lower triangular with diagonal between 1 and 2.
All inputs are finite; a program needn't handle non-finite values.
Results may differ from the reference program's by a relative error of at most 0.0055.
Values sent between devices are 32-bit elements; how exact they have to be, the bound alone decides.
A program may use at most 64 MiB of HBM per device.

```python
import math
import jax
import jax.numpy as jnp
from jax import lax

NB = 1024
BLK = 128
NI = 512
MC = 768
ITERS = 3
EB = 2
SUBS_X = 16
SUBS_Y = 16


def draw_schur(key, part):
    first, second, third = jax.random.split(jax.random.fold_in(key, 11), 3)
    logs = jax.random.uniform(first, (SUBS_X, SUBS_Y, 1, 1), jnp.float32, 0.0, math.log(30.0))
    diagonal = jax.random.uniform(second, (SUBS_X, SUBS_Y, NB), jnp.float32, 2.0, 4.0)
    noise = jnp.clip(jax.random.normal(third, (SUBS_X, SUBS_Y, NB, NB), jnp.float32), -5.0, 5.0)
    symmetric = (noise + jnp.swapaxes(noise, 2, 3)) * (0.08 / math.sqrt(2.0 * NB))
    band = -0.8 * (jnp.eye(NB, k=1, dtype=jnp.float32) + jnp.eye(NB, k=-1, dtype=jnp.float32))
    matrix = symmetric + band + diagonal[..., None] * jnp.eye(NB, dtype=jnp.float32)
    return jnp.exp(logs) * matrix


def draw_rhs_local(key, part):
    first, second = jax.random.split(jax.random.fold_in(key, 37), 2)
    level = jax.random.uniform(first, (SUBS_X, SUBS_Y, 1), jnp.float32, 2.0, 6.0)
    noise = jnp.clip(jax.random.normal(second, (SUBS_X, SUBS_Y, NB), jnp.float32), -3.0, 3.0)
    return level + noise


def draw_chol_interior(key, part):
    first, second = jax.random.split(jax.random.fold_in(key, 23), 2)
    noise = jnp.clip(jax.random.normal(first, (SUBS_X, SUBS_Y, NI, NI), jnp.float32), -2.5, 2.5)
    lower = jnp.tril(noise, -1) * (1.2 / math.sqrt(NI))
    diagonal = jax.random.uniform(second, (SUBS_X, SUBS_Y, NI), jnp.float32, 1.0, 2.0)
    return lower + diagonal[..., None] * jnp.eye(NI, dtype=jnp.float32)


def steps_of(key, extent, cuts, low, largest):
    loudness, own = 1.0, jax.random.fold_in(key, 6)
    for axis_at, parts in cuts:
        heights = jnp.exp(jax.random.uniform(jax.random.fold_in(own, axis_at), (parts,), jnp.float32, low / len(cuts), largest / len(cuts)))
        loudness = loudness * jnp.repeat(heights, extent[axis_at] // parts).reshape([-1 if axis == axis_at else 1 for axis in range(len(extent))])
    return loudness


def normal_values(rng, extent, spread, limit, pieces=(), kind=jnp.bfloat16):
    factor_of = steps_of(rng, extent, pieces, -0.22, 0.18) if pieces else 1.0
    entries = jax.random.normal(rng, extent, jnp.float32) * spread * factor_of
    return jnp.minimum(jnp.maximum(entries, -limit), limit).astype(kind)


def setup_inputs(seed: int = 0) -> dict:
    seeds = jax.random.split(jax.random.key(seed), 9)
    schur = draw_schur(jax.random.fold_in(seeds[8], 71), 0)
    rhs_local = draw_rhs_local(jax.random.fold_in(seeds[8], 71), 0)
    edge_perm = jax.vmap(lambda own: jax.random.permutation(own, EB))(jax.random.split(seeds[2], SUBS_X * SUBS_Y * 4)).reshape((SUBS_X, SUBS_Y, 4, EB)).astype(jnp.int32)
    chol_interior = draw_chol_interior(jax.random.fold_in(seeds[8], 71), 0)
    coupling = normal_values(seeds[4], (SUBS_X, SUBS_Y, NI, NB), NI ** -0.5, 0.25, ((0, 16), (1, 16)))
    boundary_diag = jnp.clip(1.0 + 2.0 * jax.random.uniform(seeds[5], (SUBS_X, SUBS_Y, NB), jnp.float32) ** steps_of(seeds[5], (SUBS_X, SUBS_Y, NB), ((0, 16), (1, 16)), -0.2, 0.2), 1.0, 3.0)
    restrict = normal_values(seeds[6], (SUBS_X, SUBS_Y, MC, NB), NB ** -0.5, 0.1875, ((0, 16), (1, 16)))
    extend = normal_values(seeds[7], (SUBS_X, SUBS_Y, NB, MC), NB ** -0.5, 0.1875, ((0, 16), (1, 16)))
    return {"schur": schur, "rhs_local": rhs_local, "edge_perm": edge_perm, "chol_interior": chol_interior, "coupling": coupling, "boundary_diag": boundary_diag, "restrict": restrict, "extend": extend}


def assemble(field, perm_hot):
    blocks = field.reshape(SUBS_X, SUBS_Y, 4, EB, BLK)
    canonical = jnp.einsum('abdkc,abdkf->abdcf', perm_hot, blocks, precision=lax.Precision.HIGHEST)
    received = jnp.stack([jnp.roll(canonical[:, :, 1], 1, axis=1), jnp.roll(canonical[:, :, 0], -1, axis=1), jnp.roll(canonical[:, :, 3], 1, axis=0), jnp.roll(canonical[:, :, 2], -1, axis=0)], axis=2)
    mapped = jnp.einsum('abdkc,abdcf->abdkf', perm_hot, received, precision=lax.Precision.HIGHEST)
    return field + mapped.reshape(SUBS_X, SUBS_Y, NB)

def inner(first, second):
    return 0.5 * jnp.sum(first * second)

def subdomain_terms(total, items):
    chol, couple, bdiag, rest, ext = items
    solved = lax.linalg.triangular_solve(chol, couple.astype(jnp.float32), left_side=True, lower=True)
    halved = lax.optimization_barrier(solved.astype(jnp.bfloat16)).astype(jnp.float32)
    gram = jnp.dot(halved.T, halved, precision=lax.Precision.HIGHEST)
    following = (jnp.diag(bdiag) - gram).astype(jnp.bfloat16)
    projected = jnp.dot(lax.optimization_barrier(following).astype(jnp.float32), ext.astype(jnp.float32), precision=lax.Precision.HIGHEST).astype(jnp.bfloat16)
    term = jnp.dot(rest.astype(jnp.float32), lax.optimization_barrier(projected).astype(jnp.float32), precision=lax.Precision.HIGHEST)
    return (total + term, following)

def reference(schur, rhs_local, edge_perm, chol_interior, coupling, boundary_diag, restrict, extend):
    perm_hot = (edge_perm[..., None] == jnp.arange(EB, dtype=jnp.int32)).astype(jnp.float32)
    right_side = assemble(rhs_local, perm_hot)
    precond = assemble(jnp.diagonal(schur, axis1=2, axis2=3), perm_hot)
    solution = jnp.zeros_like(right_side)
    residual = right_side
    scaled = residual / precond
    direction = scaled
    norm_now = inner(residual, scaled)
    for step in range(ITERS):
        local_image = jnp.einsum('abij,abj->abi', schur, direction, precision=lax.Precision.HIGHEST)
        image = assemble(local_image, perm_hot)
        step_size = norm_now / inner(direction, image)
        solution = solution + step_size * direction
        residual = residual - step_size * image
        scaled = residual / precond
        norm_next = inner(residual, scaled)
        direction = scaled + norm_next / norm_now * direction
        norm_now = norm_next
    count = SUBS_X * SUBS_Y
    items = (chol_interior.reshape(count, NI, NI), coupling.reshape(count, NI, NB), boundary_diag.reshape(count, NB), restrict.reshape(count, MC, NB), extend.reshape(count, NB, MC))
    coarse, following = lax.scan(subdomain_terms, jnp.zeros((MC, MC), jnp.float32), items)
    return (solution, residual, following.reshape(SUBS_X, SUBS_Y, NB, NB), coarse)
```

```python
import jax
import jax.numpy as jnp
from jax import lax
from jax.experimental import pallas as pl
from jax.experimental.pallas import tpu as pltpu
from jax.sharding import PartitionSpec as P

F32 = jnp.float32
BF16 = jnp.bfloat16
MESH = pl.DeviceIdType.MESH
NB = 1024
NI = 512
MC = 768
HALF = 384
Q = 96
R = 24


def dims(lhs, rhs):
    return (((lhs,), (rhs,)), ((), ()))


def split(a):
    hi = a.astype(BF16)
    lo = (a - hi.astype(F32)).astype(BF16)
    return hi, lo


def dot(a, b, dn=dims(1, 0)):
    return lax.dot_general(a, b, dn, preferred_element_type=F32)


def dot3(a, b):
    ah, al = split(a)
    bh, bl = split(b)
    return dot(ah, bh) + dot(ah, bl) + dot(al, bh)


def iota(shape, dim):
    return lax.broadcasted_iota(jnp.int32, shape, dim)


def kernel(
    perm,
    bdiag,
    rhs_hbm,
    schur_hbm,
    chol_hbm,
    coup_hbm,
    rest_hbm,
    ext_hbm,
    sol_out,
    res_out,
    next_hbm,
    coarse_out,
    rhs,
    schur,
    chol,
    coup,
    rest,
    ext,
    inv,
    xs,
    follow,
    proj,
    term,
    rawa,
    own,
    sib,
    ring1,
    mid,
    acc2,
    ring2,
    fin,
    last,
    vec,
    send0,
    recv0,
    sendx,
    recvx,
    ar_send,
    ar1,
    ar2,
    load_sem,
    out_sem,
    ex_send,
    ex_recv,
    sib_send,
    sib_recv,
    r1_send,
    r1_recv,
    r2_send,
    r2_recv,
    last_send,
    last_recv,
    a1_send,
    a1_recv,
    a2_send,
    a2_recv,
):
    a = lax.axis_index("sx")
    b = lax.axis_index("sy")
    y, zl = a // 4, a % 4
    zh, x, core = b // 8, (b // 2) % 4, b % 2
    z = zh * 4 + zl

    def device(y_, z_, x_, c_):
        return (y_ * 4 + z_ % 4, (z_ // 4) * 8 + x_ * 2 + c_)

    sibling = device(y, z, x, 1 - core)

    def plane_peer(k):
        return device((y + k // 4) % 4, z, (x + k % 4) % 4, core)

    def column_peer(k):
        return device(y, (z + k // 2) % 8, x, (core + k % 2) % 2)

    neighbours = (
        (a, (b + 15) % 16),
        (a, (b + 1) % 16),
        ((a + 15) % 16, b),
        ((a + 1) % 16, b),
    )

    loads = [
        pltpu.make_async_copy(src, dst, load_sem.at[i])
        for i, (src, dst) in enumerate(
            (
                (rhs_hbm, rhs),
                (chol_hbm, chol),
                (schur_hbm, schur),
                (coup_hbm, coup),
                (ext_hbm, ext),
                (rest_hbm, rest),
            )
        )
    ]
    for load in loads:
        load.start()

    barrier = pltpu.get_barrier_semaphore()

    def greet_plane(k, carry):
        pl.semaphore_signal(barrier, inc=1, device_id=plane_peer(k), device_id_type=MESH)
        return carry

    def greet_column(k, carry):
        pl.semaphore_signal(barrier, inc=1, device_id=column_peer(k), device_id_type=MESH)
        return carry

    for peer in neighbours:
        pl.semaphore_signal(barrier, inc=1, device_id=peer, device_id_type=MESH)
    lax.fori_loop(1, 16, greet_plane, 0)
    lax.fori_loop(1, 16, greet_column, 0)

    row = iota((8, 128), 0)
    swap = jnp.zeros((8, 128), jnp.int32)
    for d in range(4):
        swap = jnp.where(row // 2 == d, perm[d, 0], swap)

    def canonical(v):
        other = jnp.where(row % 2 == 0, pltpu.roll(v, 7, 0), pltpu.roll(v, 1, 0))
        return jnp.where(swap == 1, other, v)

    def from_edges(west, east, south, north):
        low = jnp.where(row < 4, pltpu.roll(west, 6, 0), pltpu.roll(south, 6, 0))
        high = jnp.where(row < 4, pltpu.roll(east, 2, 0), pltpu.roll(north, 2, 0))
        return canonical(jnp.where(row % 4 < 2, low, high))

    def exchange(src, dst, e):
        return [
            pltpu.make_async_remote_copy(
                src_ref=src,
                dst_ref=dst.at[d ^ 1],
                send_sem=ex_send.at[e, d],
                recv_sem=ex_recv.at[e, d ^ 1],
                device_id=neighbours[d],
                device_id_type=MESH,
            )
            for d in range(4)
        ]

    eye = iota((128, 128), 0) == iota((128, 128), 1)

    def matvec(v):
        vec[1] = v

        def body(r, carry):
            rows = pl.ds(pl.multiple_of(r * 128, 128), 128)
            total = jnp.zeros((128, 128), F32)
            for c in range(8):
                total = total + schur[rows, 128 * c : 128 * c + 128] * vec[1, c : c + 1, :]
            vec[0, pl.ds(r, 1), :] = jnp.sum(total.T, axis=0, keepdims=True)
            return carry

        lax.fori_loop(0, 8, body, 0)
        return vec[0]

    loads[0].wait()
    loads[2].wait()

    def diagonal(r, carry):
        at = pl.ds(pl.multiple_of(r * 128, 128), 128)
        vec[0, pl.ds(r, 1), :] = jnp.sum(
            jnp.where(eye, schur[at, at], 0.0), axis=0, keepdims=True
        )
        return carry

    lax.fori_loop(0, 8, diagonal, 0)
    local_rhs = rhs[...]
    local_diag = vec[0]
    send0[0:8, :] = canonical(local_rhs)
    send0[8:16, :] = canonical(local_diag)

    loads[1].wait()
    rr, cc = iota((128, 128), 0), iota((128, 128), 1)

    def invert(t):
        at = pl.ds(pl.multiple_of(t * 128, 128), 128)
        low = chol[at, at]
        on_diag = jnp.where(eye, low, 0.0)
        inv_row = 1.0 / jnp.sum(on_diag, axis=0, keepdims=True)
        inv_col = 1.0 / jnp.sum(on_diag, axis=1, keepdims=True)
        first = (rr == cc + 1) & (rr % 2 == 1)
        got = jnp.where(eye, inv_row, jnp.where(first, -(low * inv_row) * inv_col, 0.0))
        s = 2
        while s < 128:
            part = (rr // (2 * s) == cc // (2 * s)) & ((rr // s) % 2 == 1) & ((cc // s) % 2 == 0)
            got = got - dot3(got, dot3(jnp.where(part, low, 0.0), got))
            s *= 2
        return got

    blocks = [invert(t) for t in range(4)]
    for t in range(4):
        inv[128 * t : 128 * t + 128, 128 * t : 128 * t + 128] = blocks[t]

    pl.semaphore_wait(barrier, 34)
    ex0 = exchange(send0, recv0, 0)
    for copy in ex0:
        copy.start()

    for t in (0, 2):
        inv[128 * t + 128 : 128 * t + 256, 128 * t : 128 * t + 128] = -dot3(
            blocks[t + 1],
            dot3(chol[128 * t + 128 : 128 * t + 256, 128 * t : 128 * t + 128], blocks[t]),
        )
        inv[128 * t : 128 * t + 128, 128 * t + 128 : 128 * t + 256] = jnp.zeros((128, 128), F32)
    inv[256:512, 0:256] = -dot3(
        inv[256:512, 256:512], dot3(chol[256:512, 0:256], inv[0:256, 0:256])
    )

    loads[3].wait()
    top_hi, top_lo = split(inv[0:256, 0:256])
    low_hi, low_lo = split(inv[256:512, :])
    for n in range(0, NB, 256):
        up = coup[0:256, n : n + 256]
        xs[0:256, n : n + 256] = (dot(top_hi, up) + dot(top_lo, up)).astype(BF16)
        full = coup[:, n : n + 256]
        xs[256:512, n : n + 256] = (dot(low_hi, full) + dot(low_lo, full)).astype(BF16)

    def gram(m):
        at = pl.ds(pl.multiple_of(m * 256, 256), 256)
        product = dot(xs[:, at], xs[...], dims(0, 0))
        on = (iota((256, NB), 0) + m * 256) == iota((256, NB), 1)
        follow[at, :] = (jnp.where(on, bdiag[...], 0.0) - product).astype(BF16)

    def gram_range(lo, hi):
        for m in range(lo, hi):
            gram(m)

    for copy in ex0:
        copy.wait()
    assembled_rhs = local_rhs + from_edges(*(recv0[d, 0:8, :] for d in range(4)))
    precond = local_diag + from_edges(*(recv0[d, 8:16, :] for d in range(4)))
    p0 = assembled_rhs
    w0 = p0 / precond
    local0 = matvec(w0)
    sendx[0] = canonical(local0)
    ex1 = exchange(sendx.at[0], recvx.at[0], 1)
    for copy in ex1:
        copy.start()

    gram_range(0, 4)
    store = pltpu.make_async_copy(follow, next_hbm, out_sem)
    store.start()
    loads[4].wait()

    def project(h):
        proj[...] = dot(follow[...], ext[:, HALF * h : HALF * h + HALF]).astype(BF16)

    project(0)

    for copy in ex1:
        copy.wait()
    q0 = local0 + from_edges(*(recvx[0, d] for d in range(4)))
    p1 = q0 - p0
    w1 = p1 / precond
    local1 = matvec(w1)
    sendx[1] = canonical(local1)
    ex2 = exchange(sendx.at[1], recvx.at[1], 2)
    for copy in ex2:
        copy.start()

    loads[5].wait()
    sends_sib = [
        pltpu.make_async_remote_copy(
            src_ref=own.at[1 - core, h],
            dst_ref=sib.at[h],
            send_sem=sib_send.at[h],
            recv_sem=sib_recv.at[h],
            device_id=sibling,
            device_id_type=MESH,
        )
        for h in range(2)
    ]

    def terms(h):
        term[...] = dot(rest[...], proj[...])
        for k in range(16):
            rawa[R * k : R * k + R, :] = term[2 * R * k : 2 * R * k + R, :]
            own[1, h, k // 4, R * (k % 4) : R * (k % 4) + R, :] = term[
                2 * R * k + R : 2 * R * k + 2 * R, :
            ]
        flipped = rawa[...].T
        for u in range(4):
            own[0, h, u] = flipped[Q * u : Q * u + Q, :]
        sends_sib[h].start()

    terms(0)
    project(1)
    terms(1)

    for copy in ex2:
        copy.wait()
    q1 = local1 + from_edges(*(recvx[1, d] for d in range(4)))
    p2 = q1 - p1
    w2 = p2 / precond
    local2 = matvec(w2)
    sendx[2] = canonical(local2)
    ex3 = exchange(sendx.at[2], recvx.at[2], 3)
    for copy in ex3:
        copy.start()

    products = (
        0.5 * w0 * p0,
        0.5 * w0 * p1,
        0.5 * w1 * p1,
        0.5 * w1 * p2,
        0.5 * w2 * p2,
        w2 * local2,
    )
    rows = jnp.zeros((8, 128), F32)
    for i, product in enumerate(products):
        rows = jnp.where(row == i, jnp.sum(product, axis=0, keepdims=True), rows)
    sums = jnp.sum(rows, axis=1, keepdims=True)
    mine = jnp.sum(jnp.where(iota((8, 128), 1) == row, sums, 0.0), axis=0, keepdims=True)
    ar_send[0] = mine

    def gather(stage, k):
        return pltpu.make_async_remote_copy(
            src_ref=ar_send.at[stage],
            dst_ref=(ar1, ar2)[stage].at[k],
            send_sem=(a1_send, a2_send)[stage].at[k],
            recv_sem=(a1_recv, a2_recv)[stage].at[k],
            device_id=(plane_peer, column_peer)[stage](k),
            device_id_type=MESH,
        )

    def gather_start(stage):
        def body(k, carry):
            gather(stage, k).start()
            return carry

        lax.fori_loop(1, 16, body, 0)

    def gather_sum(stage, start):
        def wait(k, carry):
            gather(stage, k).wait()
            return carry

        lax.fori_loop(1, 16, wait, 0)
        total = start
        for k in range(1, 16):
            total = total + (ar1, ar2)[stage][k]
        return total

    gather_start(0)

    def ring(data, bufs, send_sem, recv_sem, along_x):
        here = jnp.where(along_x, x, y)
        right, left, across = (here + 1) % 4, (here + 3) % 4, (here + 2) % 4

        def at(place):
            return device(jnp.where(along_x, y, place), z, jnp.where(along_x, place, x), core)

        def copy(h, slot, chunk, place):
            return pltpu.make_async_remote_copy(
                src_ref=data.at[h, chunk],
                dst_ref=bufs.at[h, slot],
                send_sem=send_sem.at[h, slot],
                recv_sem=recv_sem.at[h, slot],
                device_id=at(place),
                device_id_type=MESH,
            )

        ahead = (right, left)
        behind = (left, right)

        def first(h):
            copy(h, 0, across, ahead[h]).start()
            copy(h, 1, behind[h], behind[h]).start()

        def second(h):
            copy(h, 0, across, ahead[h]).wait()
            data[h, ahead[h]] = data[h, ahead[h]] + bufs[h, 0]
            copy(h, 2, ahead[h], ahead[h]).start()

        def third(h):
            copy(h, 1, behind[h], behind[h]).wait()
            copy(h, 2, ahead[h], ahead[h]).wait()
            return data[h, here] + bufs[h, 1] + bufs[h, 2]

        return first, second, third

    mine_of = own.at[core]
    first1, second1, third1 = ring(mine_of, ring1, r1_send, r1_recv, core == 0)
    for h in range(2):
        sends_sib[h].wait()
        for u in range(4):
            mine_of[h, u] = mine_of[h, u] + sib[h, u]
        first1(h)

    total1 = gather_sum(0, ar_send[0])
    ar_send[1] = total1
    gather_start(1)

    second1(0)
    second1(1)
    first2, second2, third2 = ring(acc2, ring2, r2_send, r2_recv, core == 1)
    for h in range(2):
        mid[0:Q, :] = third1(h)
        mid[Q:128, :] = jnp.zeros((128 - Q, HALF), F32)
        turned = mid[...].T
        for v in range(4):
            acc2[h, v] = turned[Q * v : Q * v + Q, :]
        first2(h)

    moments = gather_sum(1, ar_send[1])
    lane = iota((1, 128), 1)
    g = [
        jnp.sum(jnp.where(lane == i, moments, 0.0), axis=1, keepdims=True) for i in range(6)
    ]
    g[5] = g[5] - g[4]

    def form(u, v, shift):
        total = None
        for i, ui in enumerate(u):
            for j, vj in enumerate(v):
                if ui is None or vj is None:
                    continue
                part = ui * vj * (g[i + j] + g[i + j + 1] if shift else g[i + j])
                total = part if total is None else total + part
        return total

    def plus(u, s, v):
        return [
            p if q is None else (s * q if p is None else p + s * q) for p, q in zip(u, v)
        ]

    one = jnp.ones((1, 1), F32)
    scaled = [one, None, None]
    direction = [one, None, None]
    amount = [None, None, None]
    norm = form(scaled, scaled, False)
    for step in range(3):
        size = norm / form(direction, direction, True)
        amount = plus(amount, size, direction)
        if step < 2:
            image = plus(direction, one, [None] + direction[:2])
            scaled = plus(scaled, -size, image)
            following = form(scaled, scaled, False)
            direction = plus(scaled, following / norm, direction)
            norm = following
    for copy in ex3:
        copy.wait()
    q2 = local2 + from_edges(*(recvx[2, d] for d in range(4)))
    sol_out[...] = amount[0] * w0 + amount[1] * w1 + amount[2] * w2
    res_out[...] = p0 - (amount[0] * q0 + amount[1] * q1 + amount[2] * q2)

    second2(0)
    second2(1)
    for h in range(2):
        mid[0:Q, 0:128] = third2(h)
        got = mid[:, 0:128]
        got = jnp.where(core == 1, got.T, got)
        for k in range(4):
            fin[4 * h + k] = got[R * k : R * k + R, :]

    def spread(k):
        return pltpu.make_async_remote_copy(
            src_ref=fin.at[(z + k // 2) % 8],
            dst_ref=last.at[k],
            send_sem=last_send.at[k],
            recv_sem=last_recv.at[k],
            device_id=column_peer(k),
            device_id_type=MESH,
        )

    def spread_start(k, carry):
        spread(k).start()
        return carry

    def spread_wait(k, carry):
        spread(k).wait()
        return carry

    lax.fori_loop(1, 16, spread_start, 0)
    lax.fori_loop(1, 16, spread_wait, 0)
    same = fin[z]
    for k in range(2, 16, 2):
        same = same + last[k]
    other = last[1]
    for k in range(3, 16, 2):
        other = other + last[k]
    for colour in range(2):
        rows_of = jnp.where(core == colour, same, other)
        rows_of = jnp.where(core == 0, rows_of, pltpu.roll(rows_of, 80, 1))
        coarse_out[R * colour : R * colour + R, :] = rows_of[:, 0:48]
    store.wait()


def per_device(
    schur, rhs_local, edge_perm, chol_interior, coupling, boundary_diag, restrict, extend
):
    any_ = pl.BlockSpec(memory_space=pl.ANY)
    vmem = pl.BlockSpec(memory_space=pltpu.VMEM)
    dma = pltpu.SemaphoreType.DMA
    out = pl.pallas_call(
        kernel,
        out_shape=(
            jax.ShapeDtypeStruct((8, 128), F32),
            jax.ShapeDtypeStruct((8, 128), F32),
            jax.ShapeDtypeStruct((NB, NB), BF16),
            jax.ShapeDtypeStruct((48, 48), F32),
        ),
        in_specs=[pl.BlockSpec(memory_space=pltpu.SMEM), vmem] + [any_] * 6,
        out_specs=(vmem, vmem, any_, vmem),
        scratch_shapes=[
            pltpu.VMEM((8, 128), F32),
            pltpu.VMEM((NB, NB), F32),
            pltpu.VMEM((NI, NI), F32),
            pltpu.VMEM((NI, NB), BF16),
            pltpu.VMEM((MC, NB), BF16),
            pltpu.VMEM((NB, MC), BF16),
            pltpu.VMEM((NI, NI), F32),
            pltpu.VMEM((NI, NB), BF16),
            pltpu.VMEM((NB, NB), BF16),
            pltpu.VMEM((NB, HALF), BF16),
            pltpu.VMEM((MC, HALF), F32),
            pltpu.VMEM((HALF, HALF), F32),
            pltpu.VMEM((2, 2, 4, Q, HALF), F32),
            pltpu.VMEM((2, 4, Q, HALF), F32),
            pltpu.VMEM((2, 3, Q, HALF), F32),
            pltpu.VMEM((128, HALF), F32),
            pltpu.VMEM((2, 4, Q, 128), F32),
            pltpu.VMEM((2, 3, Q, 128), F32),
            pltpu.VMEM((8, R, 128), F32),
            pltpu.VMEM((16, R, 128), F32),
            pltpu.VMEM((2, 8, 128), F32),
            pltpu.VMEM((16, 128), F32),
            pltpu.VMEM((4, 16, 128), F32),
            pltpu.VMEM((3, 8, 128), F32),
            pltpu.VMEM((3, 4, 8, 128), F32),
            pltpu.VMEM((2, 1, 128), F32),
            pltpu.VMEM((16, 1, 128), F32),
            pltpu.VMEM((16, 1, 128), F32),
            dma((6,)),
            dma,
            dma((4, 4)),
            dma((4, 4)),
            dma((2,)),
            dma((2,)),
            dma((2, 3)),
            dma((2, 3)),
            dma((2, 3)),
            dma((2, 3)),
            dma((16,)),
            dma((16,)),
            dma((16,)),
            dma((16,)),
            dma((16,)),
            dma((16,)),
        ],
        compiler_params=pltpu.CompilerParams(
            collective_id=0, has_side_effects=True, vmem_limit_bytes=60 * 1024 * 1024
        ),
        name="interface_and_coarse",
    )(
        edge_perm[0, 0],
        boundary_diag[0],
        rhs_local.reshape(8, 128),
        schur[0, 0],
        chol_interior[0, 0],
        coupling[0, 0],
        restrict[0, 0],
        extend[0, 0],
    )
    sol, res, following, coarse = out
    return sol.reshape(1, 1, NB), res.reshape(1, 1, NB), following[None, None], coarse


def solution(mesh):
    wide = P("sx", "sy", None, None)
    flat = P("sx", "sy", None)
    return jax.shard_map(
        per_device,
        mesh=mesh,
        in_specs=(wide, flat, wide, wide, wide, flat, wide, wide),
        out_specs=(flat, flat, wide, P("sx", "sy")),
        check_vma=False,
    )
```

```python
import jax
import jax.numpy as jnp
from jax import lax
from jax.experimental import pallas as pl
from jax.experimental.pallas import tpu as pltpu
from jax.sharding import PartitionSpec as P

F32 = jnp.float32
BF16 = jnp.bfloat16
MESH = pl.DeviceIdType.MESH
NB = 1024
NI = 512
MC = 768
HALF = 384
Q = 96
R = 24


def dims(lhs, rhs):
    return (((lhs,), (rhs,)), ((), ()))


def split(a):
    hi = a.astype(BF16)
    lo = (a - hi.astype(F32)).astype(BF16)
    return hi, lo


def dot(a, b, dn=dims(1, 0)):
    return lax.dot_general(a, b, dn, preferred_element_type=F32)


def dot3(a, b):
    ah, al = split(a)
    bh, bl = split(b)
    return dot(ah, bh) + dot(ah, bl) + dot(al, bh)


def dot3_packed(a, b):
    ah, al = split(a)
    bh, bl = split(b)
    lhs = jnp.concatenate([ah, al], axis=1)
    rhs = jnp.concatenate(
        [
            jnp.concatenate([bh, bl], axis=1),
            jnp.concatenate([bh, jnp.zeros_like(bl)], axis=1),
        ],
        axis=0,
    )
    both = dot(lhs, rhs)
    return both[:, 0:128] + both[:, 128:256]


def iota(shape, dim):
    return lax.broadcasted_iota(jnp.int32, shape, dim)


def kernel(
    perm_hbm,
    bdiag_hbm,
    rhs_hbm,
    schur_hbm,
    chol_hbm,
    coup_hbm,
    rest_hbm,
    ext_hbm,
    sol_out,
    res_out,
    next_hbm,
    coarse_out,
    perm,
    bdiag,
    rhs,
    schur,
    chol,
    coup,
    rest,
    ext,
    inv,
    xs,
    follow,
    proj,
    term,
    rawa,
    own,
    sib,
    ring1,
    mid,
    acc2,
    ring2,
    fin,
    last,
    vec,
    send0,
    recv0,
    sendx,
    recvx,
    ar_send,
    ar1,
    ar2,
    load_sem,
    out_sem,
    ex_send,
    ex_recv,
    sib_send,
    sib_recv,
    r1_send,
    r1_recv,
    r2_send,
    r2_recv,
    last_send,
    last_recv,
    a1_send,
    a1_recv,
    a2_send,
    a2_recv,
):
    a = lax.axis_index("sx")
    b = lax.axis_index("sy")
    y, zl = a // 4, a % 4
    zh, x, core = b // 8, (b // 2) % 4, b % 2
    z = zh * 4 + zl

    def device(y_, z_, x_, c_):
        return (y_ * 4 + z_ % 4, (z_ // 4) * 8 + x_ * 2 + c_)

    sibling = device(y, z, x, 1 - core)

    def plane_peer(k):
        return device((y + k // 4) % 4, z, (x + k % 4) % 4, core)

    def column_peer(k):
        return device(y, (z + k // 2) % 8, x, (core + k % 2) % 2)

    neighbours = (
        (a, (b + 15) % 16),
        (a, (b + 1) % 16),
        ((a + 15) % 16, b),
        ((a + 1) % 16, b),
    )

    loads = [
        pltpu.make_async_copy(src, dst, load_sem.at[i])
        for i, (src, dst) in enumerate(
            (
                (rhs_hbm, rhs),
                (chol_hbm, chol),
                (schur_hbm, schur),
                (coup_hbm, coup),
                (ext_hbm, ext),
                (rest_hbm, rest),
                (perm_hbm, perm),
                (bdiag_hbm, bdiag),
            )
        )
    ]
    for i in (6, 0, 1, 2, 3, 7, 4, 5):
        loads[i].start()

    barrier = pltpu.get_barrier_semaphore()

    def greet_plane(k, carry):
        pl.semaphore_signal(barrier, inc=1, device_id=plane_peer(k), device_id_type=MESH)
        return carry

    def greet_column(k, carry):
        pl.semaphore_signal(barrier, inc=1, device_id=column_peer(k), device_id_type=MESH)
        return carry

    for peer in neighbours:
        pl.semaphore_signal(barrier, inc=1, device_id=peer, device_id_type=MESH)
    lax.fori_loop(1, 16, greet_plane, 0)
    lax.fori_loop(1, 16, greet_column, 0)

    row = iota((8, 128), 0)

    def canonical(v):
        other = jnp.where(row % 2 == 0, pltpu.roll(v, 7, 0), pltpu.roll(v, 1, 0))
        return jnp.where(swap == 1, other, v)

    def from_edges(west, east, south, north):
        low = jnp.where(row < 4, pltpu.roll(west, 6, 0), pltpu.roll(south, 6, 0))
        high = jnp.where(row < 4, pltpu.roll(east, 2, 0), pltpu.roll(north, 2, 0))
        return canonical(jnp.where(row % 4 < 2, low, high))

    def exchange(src, dst, e):
        return [
            pltpu.make_async_remote_copy(
                src_ref=src,
                dst_ref=dst.at[d ^ 1],
                send_sem=ex_send.at[e, d],
                recv_sem=ex_recv.at[e, d ^ 1],
                device_id=neighbours[d],
                device_id_type=MESH,
            )
            for d in range(4)
        ]

    eye = iota((128, 128), 0) == iota((128, 128), 1)

    def matvec(v):
        vec[1] = v

        def body(r, carry):
            rows = pl.ds(pl.multiple_of(r * 128, 128), 128)
            total = jnp.zeros((128, 128), F32)
            for c in range(8):
                total = total + schur[rows, 128 * c : 128 * c + 128] * vec[1, c : c + 1, :]
            vec[0, pl.ds(r, 1), :] = jnp.sum(total.T, axis=0, keepdims=True)
            return carry

        lax.fori_loop(0, 8, body, 0)
        return vec[0]

    rr, cc = iota((128, 128), 0), iota((128, 128), 1)
    group, place = iota((8, 128), 1) // 8, iota((8, 128), 1) % 8

    def base(t):
        packed = jnp.zeros((8, 128), F32)
        for k in range(16):
            at = 128 * t + 8 * k
            packed = jnp.where(group == k, chol[at : at + 8, 128 * t : 128 * t + 128], packed)
        columns = []
        pivots = jnp.ones((8, 128), F32)
        for j in range(8):
            column = jnp.where(place == j, packed, 0.0)
            if j:
                column = pltpu.roll(column, 128 - j, 1)
            for step in (1, 2, 4):
                column = column + pltpu.roll(column, step, 1)
            pivots = jnp.where(row == j, column, pivots)
            columns.append(jnp.where(row > j, column, 0.0))
        pivots = 1.0 / pivots
        got = jnp.where(place == row, 1.0, 0.0)
        for j in range(8):
            line = got[j : j + 1, :] * pivots[j : j + 1, :]
            got = jnp.where(row == j, line, got - columns[j] * line)
        return jnp.concatenate([jnp.where(group == k, got, 0.0) for k in range(16)], axis=0)

    loads[1].wait()
    blocks = [base(t) for t in range(4)]

    loads[0].wait()
    loads[2].wait()
    loads[6].wait()
    swap = jnp.zeros((8, 128), jnp.int32)
    for d in range(4):
        swap = jnp.where(row // 2 == d, perm[0, d], swap)


    def diagonal(r, carry):
        at = pl.ds(pl.multiple_of(r * 128, 128), 128)
        vec[0, pl.ds(r, 1), :] = jnp.sum(
            jnp.where(eye, schur[at, at], 0.0), axis=0, keepdims=True
        )
        return carry

    lax.fori_loop(0, 8, diagonal, 0)
    local_rhs = rhs[...]
    local_diag = vec[0]
    send0[0:8, :] = canonical(local_rhs)
    send0[8:16, :] = canonical(local_diag)

    pl.semaphore_wait(barrier, 34)
    ex0 = exchange(send0, recv0, 0)
    for copy in ex0:
        copy.start()

    for s in (8, 16, 32, 64):
        part = (rr // (2 * s) == cc // (2 * s)) & ((rr // s) % 2 == 1) & ((cc // s) % 2 == 0)
        inner = [
            dot3_packed(
                jnp.where(part, chol[128 * t : 128 * t + 128, 128 * t : 128 * t + 128], 0.0),
                blocks[t],
            )
            for t in range(4)
        ]
        blocks = [blocks[t] - dot3_packed(blocks[t], inner[t]) for t in range(4)]
    for t in range(4):
        inv[128 * t : 128 * t + 128, 128 * t : 128 * t + 128] = blocks[t]
    for t in (0, 2):
        inv[128 * t + 128 : 128 * t + 256, 128 * t : 128 * t + 128] = -dot3_packed(
            blocks[t + 1],
            dot3_packed(chol[128 * t + 128 : 128 * t + 256, 128 * t : 128 * t + 128], blocks[t]),
        )
        inv[128 * t : 128 * t + 128, 128 * t + 128 : 128 * t + 256] = jnp.zeros((128, 128), F32)
    inv[256:512, 0:256] = -dot3(
        inv[256:512, 256:512], dot3(chol[256:512, 0:256], inv[0:256, 0:256])
    )

    loads[3].wait()
    top_hi, top_lo = split(inv[0:256, 0:256])
    low_hi, low_lo = split(inv[256:512, :])
    for n in range(0, NB, 256):
        up = coup[0:256, n : n + 256]
        xs[0:256, n : n + 256] = (dot(top_hi, up) + dot(top_lo, up)).astype(BF16)
        full = coup[:, n : n + 256]
        xs[256:512, n : n + 256] = (dot(low_hi, full) + dot(low_lo, full)).astype(BF16)

    def gram(m):
        at = pl.ds(pl.multiple_of(m * 256, 256), 256)
        product = dot(xs[:, at], xs[...], dims(0, 0))
        on = (iota((256, NB), 0) + m * 256) == iota((256, NB), 1)
        follow[at, :] = (jnp.where(on, bdiag[...], 0.0) - product).astype(BF16)

    def gram_range(lo, hi):
        for m in range(lo, hi):
            gram(m)

    for copy in ex0:
        copy.wait()
    assembled_rhs = local_rhs + from_edges(*(recv0[d, 0:8, :] for d in range(4)))
    precond = local_diag + from_edges(*(recv0[d, 8:16, :] for d in range(4)))
    p0 = assembled_rhs
    w0 = p0 / precond
    local0 = matvec(w0)
    sendx[0] = canonical(local0)
    ex1 = exchange(sendx.at[0], recvx.at[0], 1)
    for copy in ex1:
        copy.start()

    loads[7].wait()
    gram_range(0, 4)
    store = pltpu.make_async_copy(follow, next_hbm, out_sem)
    store.start()
    loads[4].wait()

    def project(h):
        proj[...] = dot(follow[...], ext[:, HALF * h : HALF * h + HALF]).astype(BF16)

    loads[5].wait()
    sends_sib = [
        pltpu.make_async_remote_copy(
            src_ref=own.at[1 - core, h],
            dst_ref=sib.at[h],
            send_sem=sib_send.at[h],
            recv_sem=sib_recv.at[h],
            device_id=sibling,
            device_id_type=MESH,
        )
        for h in range(2)
    ]

    def terms(h):
        term[...] = dot(rest[...], proj[...])
        for k in range(16):
            rawa[R * k : R * k + R, :] = term[2 * R * k : 2 * R * k + R, :]
            own[1, h, k // 4, R * (k % 4) : R * (k % 4) + R, :] = term[
                2 * R * k + R : 2 * R * k + 2 * R, :
            ]
        flipped = rawa[...].T
        for u in range(4):
            own[0, h, u] = flipped[Q * u : Q * u + Q, :]
        sends_sib[h].start()

    place1 = jnp.where(core == 0, x, y)
    place2 = jnp.where(core == 0, y, x)

    def on_ring(is_x, at):
        return device(jnp.where(is_x, y, at), z, jnp.where(is_x, at, x), core)

    data = own.at[core]
    ahead = ((place1 + 1) % 4, (place1 + 3) % 4)
    behind = ((place1 + 3) % 4, (place1 + 1) % 4)
    across = (place1 + 2) % 4
    PART = Q // 2

    def copy1(h, slot):
        if slot == 4:
            src, dst, to = data.at[h, behind[h]], ring1.at[h, 2], behind[h]
        else:
            chunk = across if slot < 2 else ahead[h]
            part = pl.ds(PART * (slot % 2), PART)
            src, dst, to = data.at[h, chunk, part], ring1.at[h, slot // 2, part], ahead[h]
        return pltpu.make_async_remote_copy(
            src_ref=src,
            dst_ref=dst,
            send_sem=r1_send.at[h, slot],
            recv_sem=r1_recv.at[h, slot],
            device_id=on_ring(core == 0, to),
            device_id_type=MESH,
        )

    def join(h):
        sends_sib[h].wait()
        for u in range(4):
            data[h, u] = data[h, u] + sib[h, u]
        copy1(h, 0).start()
        copy1(h, 1).start()

    def pass_on(h):
        for i in range(2):
            part = pl.ds(PART * i, PART)
            copy1(h, i).wait()
            data[h, ahead[h], part] = data[h, ahead[h], part] + ring1[h, 0, part]
            copy1(h, 2 + i).start()

    def copy2(h, k):
        to = (place2 + k) % 4
        return pltpu.make_async_remote_copy(
            src_ref=acc2.at[h, to],
            dst_ref=ring2.at[h, k - 1],
            send_sem=r2_send.at[h, k - 1],
            recv_sem=r2_recv.at[h, k - 1],
            device_id=on_ring(core == 1, to),
            device_id_type=MESH,
        )

    def turn(h):
        for slot in (2, 3, 4):
            copy1(h, slot).wait()
        mid[0:Q, :] = data[h, place1] + ring1[h, 1] + ring1[h, 2]
        mid[Q:128, :] = jnp.zeros((128 - Q, HALF), F32)
        turned = mid[...].T
        for v in range(4):
            acc2[h, v] = turned[Q * v : Q * v + Q, :]
        for k in (2, 1, 3):
            copy2(h, k).start()

    me = z * 2 + core

    def spread(to, source):
        return pltpu.make_async_remote_copy(
            src_ref=fin.at[to // 2],
            dst_ref=last.at[source],
            send_sem=last_send.at[to],
            recv_sem=last_recv.at[source],
            device_id=device(y, to // 2, x, to % 2),
            device_id_type=MESH,
        )

    def settle(h):
        for k in (1, 2, 3):
            copy2(h, k).wait()
        mid[0:Q, 0:128] = acc2[h, place2] + ring2[h, 0] + ring2[h, 1] + ring2[h, 2]
        got = mid[:, 0:128]
        got = jnp.where(core == 1, got.T, got)
        for k in range(4):
            fin[4 * h + k] = got[R * k : R * k + R, :]

        def start(k, carry):
            @pl.when(k != me)
            def _():
                spread(k, me).start()

            return carry

        lax.fori_loop(8 * h, 8 * h + 8, start, 0)

    project(0)
    terms(0)
    project(1)
    terms(1)
    join(0)
    copy1(0, 4).start()

    for copy in ex1:
        copy.wait()
    q0 = local0 + from_edges(*(recvx[0, d] for d in range(4)))
    p1 = q0 - p0
    w1 = p1 / precond
    local1 = matvec(w1)
    sendx[1] = canonical(local1)
    ex2 = exchange(sendx.at[1], recvx.at[1], 2)
    for copy in ex2:
        copy.start()

    join(1)
    pass_on(0)
    copy1(1, 4).start()
    pass_on(1)
    turn(0)

    for copy in ex2:
        copy.wait()
    q1 = local1 + from_edges(*(recvx[1, d] for d in range(4)))
    p2 = q1 - p1
    w2 = p2 / precond
    local2 = matvec(w2)
    sendx[2] = canonical(local2)
    ex3 = exchange(sendx.at[2], recvx.at[2], 3)
    for copy in ex3:
        copy.start()

    products = (
        0.5 * w0 * p0,
        0.5 * w0 * p1,
        0.5 * w1 * p1,
        0.5 * w1 * p2,
        0.5 * w2 * p2,
        w2 * local2,
    )
    rows = jnp.zeros((8, 128), F32)
    for i, product in enumerate(products):
        rows = jnp.where(row == i, jnp.sum(product, axis=0, keepdims=True), rows)
    sums = jnp.sum(rows, axis=1, keepdims=True)
    mine = jnp.sum(jnp.where(iota((8, 128), 1) == row, sums, 0.0), axis=0, keepdims=True)
    ar_send[0] = mine

    def gather(stage, k):
        return pltpu.make_async_remote_copy(
            src_ref=ar_send.at[stage],
            dst_ref=(ar1, ar2)[stage].at[k],
            send_sem=(a1_send, a2_send)[stage].at[k],
            recv_sem=(a1_recv, a2_recv)[stage].at[k],
            device_id=(plane_peer, column_peer)[stage](k),
            device_id_type=MESH,
        )

    def gather_start(stage):
        def body(k, carry):
            gather(stage, k).start()
            return carry

        lax.fori_loop(1, 16, body, 0)

    def gather_sum(stage, start):
        def wait(k, carry):
            gather(stage, k).wait()
            return carry

        lax.fori_loop(1, 16, wait, 0)
        total = start
        for k in range(1, 16):
            total = total + (ar1, ar2)[stage][k]
        return total

    gather_start(0)

    turn(1)
    settle(0)
    total1 = gather_sum(0, ar_send[0])
    ar_send[1] = total1
    gather_start(1)
    settle(1)
    last[me] = fin[z]

    moments = gather_sum(1, ar_send[1])
    lane = iota((1, 128), 1)
    g = [
        jnp.sum(jnp.where(lane == i, moments, 0.0), axis=1, keepdims=True) for i in range(6)
    ]
    g[5] = g[5] - g[4]

    def form(u, v, shift):
        total = None
        for i, ui in enumerate(u):
            for j, vj in enumerate(v):
                if ui is None or vj is None:
                    continue
                part = ui * vj * (g[i + j] + g[i + j + 1] if shift else g[i + j])
                total = part if total is None else total + part
        return total

    def plus(u, s, v):
        return [
            p if q is None else (s * q if p is None else p + s * q) for p, q in zip(u, v)
        ]

    one = jnp.ones((1, 1), F32)
    scaled = [one, None, None]
    direction = [one, None, None]
    amount = [None, None, None]
    norm = form(scaled, scaled, False)
    for step in range(3):
        size = norm / form(direction, direction, True)
        amount = plus(amount, size, direction)
        if step < 2:
            image = plus(direction, one, [None] + direction[:2])
            scaled = plus(scaled, -size, image)
            following = form(scaled, scaled, False)
            direction = plus(scaled, following / norm, direction)
            norm = following
    for copy in ex3:
        copy.wait()
    q2 = local2 + from_edges(*(recvx[2, d] for d in range(4)))
    sol_out[...] = amount[0] * w0 + amount[1] * w1 + amount[2] * w2
    res_out[...] = p0 - (amount[0] * q0 + amount[1] * q1 + amount[2] * q2)


    def finish(k, carry):
        @pl.when(k != me)
        def _():
            spread(k, k).wait()

        return carry

    lax.fori_loop(0, 16, finish, 0)
    for colour in range(2):
        rows_of = last[colour]
        for k in range(1, 8):
            rows_of = rows_of + last[2 * k + colour]
        rows_of = jnp.where(core == 0, rows_of, pltpu.roll(rows_of, 80, 1))
        coarse_out[R * colour : R * colour + R, :] = rows_of[:, 0:48]
    store.wait()


def store_outputs(
    sol, res, follow_in, coarse, sol_out, res_out, next_hbm, coarse_out, out_sem
):
    part = NB // 4
    rows = [pl.ds(part * i, part) for i in range(4)]
    back = [
        pltpu.make_async_copy(follow_in.at[rows[i]], next_hbm.at[0, 0, rows[i]], out_sem.at[i])
        for i in range(4)
    ]
    for copy in back:
        copy.start()
    for k in range(8):
        sol_out[0, 0:1, 128 * k : 128 * k + 128] = sol[k : k + 1, :]
        res_out[0, 0:1, 128 * k : 128 * k + 128] = res[k : k + 1, :]
    coarse_out[...] = coarse[...]
    for copy in back:
        copy.wait()


def per_device(
    schur, rhs_local, edge_perm, chol_interior, coupling, boundary_diag, restrict, extend
):
    any_ = pl.BlockSpec(memory_space=pl.ANY)
    vmem = pl.BlockSpec(memory_space=pltpu.VMEM)
    dma = pltpu.SemaphoreType.DMA
    out = pl.pallas_call(
        kernel,
        out_shape=(
            jax.ShapeDtypeStruct((8, 128), F32),
            jax.ShapeDtypeStruct((8, 128), F32),
            jax.ShapeDtypeStruct((NB, NB), BF16),
            jax.ShapeDtypeStruct((48, 48), F32),
        ),
        in_specs=[pl.BlockSpec(memory_space=pltpu.HBM)] * 8,
        out_specs=(vmem, vmem, any_, vmem),
        scratch_shapes=[
            pltpu.SMEM((2, 4), jnp.int32),
            pltpu.VMEM((1, NB), F32),
            pltpu.VMEM((8, 128), F32),
            pltpu.VMEM((NB, NB), F32),
            pltpu.VMEM((NI, NI), F32),
            pltpu.VMEM((NI, NB), BF16),
            pltpu.VMEM((MC, NB), BF16),
            pltpu.VMEM((NB, MC), BF16),
            pltpu.VMEM((NI, NI), F32),
            pltpu.VMEM((NI, NB), BF16),
            pltpu.VMEM((NB, NB), BF16),
            pltpu.VMEM((NB, HALF), BF16),
            pltpu.VMEM((MC, HALF), F32),
            pltpu.VMEM((HALF, HALF), F32),
            pltpu.VMEM((2, 2, 4, Q, HALF), F32),
            pltpu.VMEM((2, 4, Q, HALF), F32),
            pltpu.VMEM((2, 3, Q, HALF), F32),
            pltpu.VMEM((128, HALF), F32),
            pltpu.VMEM((2, 4, Q, 128), F32),
            pltpu.VMEM((2, 3, Q, 128), F32),
            pltpu.VMEM((8, R, 128), F32),
            pltpu.VMEM((16, R, 128), F32),
            pltpu.VMEM((2, 8, 128), F32),
            pltpu.VMEM((16, 128), F32),
            pltpu.VMEM((4, 16, 128), F32),
            pltpu.VMEM((3, 8, 128), F32),
            pltpu.VMEM((3, 4, 8, 128), F32),
            pltpu.VMEM((2, 1, 128), F32),
            pltpu.VMEM((16, 1, 128), F32),
            pltpu.VMEM((16, 1, 128), F32),
            dma((8,)),
            dma,
            dma((4, 4)),
            dma((4, 4)),
            dma((2,)),
            dma((2,)),
            dma((2, 5)),
            dma((2, 5)),
            dma((2, 3)),
            dma((2, 3)),
            dma((16,)),
            dma((16,)),
            dma((16,)),
            dma((16,)),
            dma((16,)),
            dma((16,)),
        ],
        compiler_params=pltpu.CompilerParams(
            collective_id=0, has_side_effects=True, vmem_limit_bytes=36 * 1024 * 1024
        ),
        name="interface_and_coarse",
    )(
        *(
            pltpu.with_memory_space_constraint(array, pltpu.HBM)
            for array in (
                edge_perm[0, 0].T,
                boundary_diag[0],
                rhs_local.reshape(8, 128),
                schur[0, 0],
                chol_interior[0, 0],
                coupling[0, 0],
                restrict[0, 0],
                extend[0, 0],
            )
        )
    )
    return pl.pallas_call(
        store_outputs,
        out_shape=(
            jax.ShapeDtypeStruct((1, 1, NB), F32),
            jax.ShapeDtypeStruct((1, 1, NB), F32),
            jax.ShapeDtypeStruct((1, 1, NB, NB), BF16),
            jax.ShapeDtypeStruct((48, 48), F32),
        ),
        in_specs=[vmem, vmem, any_, vmem],
        out_specs=(vmem, vmem, any_, vmem),
        scratch_shapes=[dma((4,))],
        compiler_params=pltpu.CompilerParams(vmem_limit_bytes=4 * 1024 * 1024),
        name="store_outputs",
    )(*out)


def solution(mesh):
    wide = P("sx", "sy", None, None)
    flat = P("sx", "sy", None)
    return jax.shard_map(
        per_device,
        mesh=mesh,
        in_specs=(wide, flat, wide, wide, wide, flat, wide, wide),
        out_specs=(flat, flat, wide, P("sx", "sy")),
        check_vma=False,
    )
```

```python
import jax
import jax.numpy as jnp
from jax import lax
from jax.experimental import pallas as pl
from jax.experimental.pallas import tpu as pltpu
from jax.sharding import PartitionSpec as P

F32 = jnp.float32
BF16 = jnp.bfloat16
MESH = pl.DeviceIdType.MESH
NB = 1024
NI = 512
MC = 768
HALF = 384
Q = 96
R = 24


def dims(lhs, rhs):
    return (((lhs,), (rhs,)), ((), ()))


def split(a):
    hi = a.astype(BF16)
    lo = (a - hi.astype(F32)).astype(BF16)
    return hi, lo


def dot(a, b, dn=dims(1, 0)):
    return lax.dot_general(a, b, dn, preferred_element_type=F32)


def dot3(a, b):
    ah, al = split(a)
    bh, bl = split(b)
    return dot(ah, bh) + dot(ah, bl) + dot(al, bh)


def dot3_packed(a, b):
    ah, al = split(a)
    bh, bl = split(b)
    lhs = jnp.concatenate([ah, al], axis=1)
    rhs = jnp.concatenate(
        [
            jnp.concatenate([bh, bl], axis=1),
            jnp.concatenate([bh, jnp.zeros_like(bl)], axis=1),
        ],
        axis=0,
    )
    both = dot(lhs, rhs)
    return both[:, 0:128] + both[:, 128:256]


def iota(shape, dim):
    return lax.broadcasted_iota(jnp.int32, shape, dim)


def kernel(
    perm_hbm,
    bdiag_hbm,
    rhs_hbm,
    schur_hbm,
    chol_hbm,
    coup_hbm,
    rest_hbm,
    ext_hbm,
    sol_out,
    res_out,
    next_hbm,
    coarse_out,
    perm,
    bdiag,
    rhs,
    corner,
    schur,
    chol,
    coup,
    rest,
    ext,
    inv,
    xs,
    follow,
    proj,
    rawa,
    own,
    sib,
    ring1,
    mid,
    acc2,
    ring2,
    fin,
    last,
    vec,
    sol,
    res,
    coarse,
    send0,
    recv0,
    sendx,
    recvx,
    ar_send,
    ar1,
    ar2,
    load_sem,
    corner_sem,
    out_sem,
    result_sem,
    ex_send,
    ex_recv,
    sib_send,
    sib_recv,
    r1_send,
    r1_recv,
    r2_send,
    r2_recv,
    last_send,
    last_recv,
    a1_send,
    a1_recv,
    a2_send,
    a2_recv,
):
    a = lax.axis_index("sx")
    b = lax.axis_index("sy")
    y, zl = a // 4, a % 4
    zh, x, core = b // 8, (b // 2) % 4, b % 2
    z = zh * 4 + zl

    def device(y_, z_, x_, c_):
        return (y_ * 4 + z_ % 4, (z_ // 4) * 8 + x_ * 2 + c_)

    sibling = device(y, z, x, 1 - core)

    def plane_peer(k):
        return device((y + k // 4) % 4, z, (x + k % 4) % 4, core)

    def column_peer(k):
        return device(y, (z + k // 2) % 8, x, (core + k % 2) % 2)

    neighbours = (
        (a, (b + 15) % 16),
        (a, (b + 1) % 16),
        ((a + 15) % 16, b),
        ((a + 1) % 16, b),
    )

    barrier = pltpu.get_barrier_semaphore()
    for peer in neighbours:
        pl.semaphore_signal(barrier, inc=1, device_id=peer, device_id_type=MESH)
    for k in range(1, 16):
        pl.semaphore_signal(barrier, inc=1, device_id=column_peer(k), device_id_type=MESH)
        pl.semaphore_signal(barrier, inc=1, device_id=plane_peer(k), device_id_type=MESH)

    loads = [
        pltpu.make_async_copy(src, dst, load_sem.at[i])
        for i, (src, dst) in enumerate(
            (
                (rhs_hbm, rhs),
                (chol_hbm, chol),
                (schur_hbm, schur),
                (coup_hbm, coup),
                (ext_hbm, ext),
                (rest_hbm, rest),
                (perm_hbm, perm),
                (bdiag_hbm, bdiag),
            )
        )
    ]
    corners = [
        pltpu.make_async_copy(
            schur_hbm.at[pl.ds(128 * r, 128), pl.ds(128 * r, 128)], corner.at[r], corner_sem.at[r]
        )
        for r in range(8)
    ]
    for i in (6, 0, 1):
        loads[i].start()
    for copy in corners:
        copy.start()

    row = iota((8, 128), 0)

    def canonical(v):
        other = jnp.where(row % 2 == 0, pltpu.roll(v, 7, 0), pltpu.roll(v, 1, 0))
        return jnp.where(swap == 1, other, v)

    def from_edges(west, east, south, north):
        low = jnp.where(row < 4, pltpu.roll(west, 6, 0), pltpu.roll(south, 6, 0))
        high = jnp.where(row < 4, pltpu.roll(east, 2, 0), pltpu.roll(north, 2, 0))
        return canonical(jnp.where(row % 4 < 2, low, high))

    def exchange(src, dst, e):
        return [
            pltpu.make_async_remote_copy(
                src_ref=src,
                dst_ref=dst.at[d ^ 1],
                send_sem=ex_send.at[e, d],
                recv_sem=ex_recv.at[e, d ^ 1],
                device_id=neighbours[d],
                device_id_type=MESH,
            )
            for d in range(4)
        ]

    eye = iota((128, 128), 0) == iota((128, 128), 1)

    def matvec(v):
        vec[1] = v

        for r in range(8):
            total = jnp.zeros((128, 128), F32)
            for c in range(8):
                total = (
                    total
                    + schur[128 * r : 128 * r + 128, 128 * c : 128 * c + 128]
                    * vec[1, c : c + 1, :]
                )
            vec[0, r : r + 1, :] = jnp.sum(total.T, axis=0, keepdims=True)
        return vec[0]

    rr, cc = iota((128, 128), 0), iota((128, 128), 1)
    group, place = iota((8, 128), 1) // 8, iota((8, 128), 1) % 8

    def base(t):
        packed = jnp.zeros((8, 128), F32)
        for k in range(16):
            at = 128 * t + 8 * k
            packed = jnp.where(group == k, chol[at : at + 8, 128 * t : 128 * t + 128], packed)
        columns = []
        pivots = jnp.ones((8, 128), F32)
        for j in range(8):
            column = jnp.where(place == j, packed, 0.0)
            if j:
                column = pltpu.roll(column, 128 - j, 1)
            for step in (1, 2, 4):
                column = column + pltpu.roll(column, step, 1)
            pivots = jnp.where(row == j, column, pivots)
            columns.append(jnp.where(row > j, column, 0.0))
        pivots = 1.0 / pivots
        got = jnp.where(place == row, 1.0, 0.0)
        for j in range(8):
            line = got[j : j + 1, :] * pivots[j : j + 1, :]
            got = jnp.where(row == j, line, got - columns[j] * line)
        return jnp.concatenate([jnp.where(group == k, got, 0.0) for k in range(16)], axis=0)

    loads[1].wait()
    blocks = [base(t) for t in range(4)]

    loads[0].wait()
    loads[6].wait()
    swap = jnp.zeros((8, 128), jnp.int32)
    for d in range(4):
        swap = jnp.where(row // 2 == d, perm[0, d], swap)


    for copy in corners:
        copy.wait()
    for i in (3, 2, 7, 4, 5):
        loads[i].start()
    for r in range(8):
        vec[0, r : r + 1, :] = jnp.sum(jnp.where(eye, corner[r], 0.0), axis=0, keepdims=True)
    local_rhs = rhs[...]
    local_diag = vec[0]
    send0[0:8, :] = canonical(local_rhs)
    send0[8:16, :] = canonical(local_diag)

    pl.semaphore_wait(barrier, 34)
    ex0 = exchange(send0, recv0, 0)
    for copy in ex0:
        copy.start()

    for s in (8, 16, 32, 64):
        part = (rr // (2 * s) == cc // (2 * s)) & ((rr // s) % 2 == 1) & ((cc // s) % 2 == 0)
        inner = [
            dot3_packed(
                jnp.where(part, chol[128 * t : 128 * t + 128, 128 * t : 128 * t + 128], 0.0),
                blocks[t],
            )
            for t in range(4)
        ]
        blocks = [blocks[t] - dot3_packed(blocks[t], inner[t]) for t in range(4)]
    for t in range(4):
        inv[128 * t : 128 * t + 128, 128 * t : 128 * t + 128] = blocks[t]
    for t in (0, 2):
        inv[128 * t + 128 : 128 * t + 256, 128 * t : 128 * t + 128] = -dot3_packed(
            blocks[t + 1],
            dot3_packed(chol[128 * t + 128 : 128 * t + 256, 128 * t : 128 * t + 128], blocks[t]),
        )
        inv[128 * t : 128 * t + 128, 128 * t + 128 : 128 * t + 256] = jnp.zeros((128, 128), F32)
    inv[256:512, 0:256] = -dot3(
        inv[256:512, 256:512], dot3(chol[256:512, 0:256], inv[0:256, 0:256])
    )

    loads[3].wait()
    top_hi, top_lo = split(inv[0:256, 0:256])
    low_hi, low_lo = split(inv[256:512, :])
    for n in range(0, NB, 256):
        up = coup[0:256, n : n + 256]
        xs[0:256, n : n + 256] = (dot(top_hi, up) + dot(top_lo, up)).astype(BF16)
        full = coup[:, n : n + 256]
        xs[256:512, n : n + 256] = (dot(low_hi, full) + dot(low_lo, full)).astype(BF16)

    def gram(m):
        at = pl.ds(pl.multiple_of(m * 256, 256), 256)
        product = dot(xs[:, at], xs[...], dims(0, 0))
        on = (iota((256, NB), 0) + m * 256) == iota((256, NB), 1)
        follow[at, :] = (jnp.where(on, bdiag[...], 0.0) - product).astype(BF16)

    def gram_range(lo, hi):
        for m in range(lo, hi):
            gram(m)

    loads[7].wait()
    gram_range(0, 4)

    for copy in ex0:
        copy.wait()
    loads[2].wait()
    assembled_rhs = local_rhs + from_edges(*(recv0[d, 0:8, :] for d in range(4)))
    precond = local_diag + from_edges(*(recv0[d, 8:16, :] for d in range(4)))
    p0 = assembled_rhs
    w0 = p0 / precond
    local0 = matvec(w0)
    sendx[0] = canonical(local0)
    ex1 = exchange(sendx.at[0], recvx.at[0], 1)
    for copy in ex1:
        copy.start()

    store = pltpu.make_async_copy(follow, next_hbm, out_sem)
    store.start()
    loads[4].wait()

    loads[5].wait()
    PART = Q // 2

    def to_sibling(h, i):
        part = pl.ds(PART * i, PART)
        return pltpu.make_async_remote_copy(
            src_ref=own.at[1 - core, h, :, part],
            dst_ref=sib.at[h, :, part],
            send_sem=sib_send.at[h, i],
            recv_sem=sib_recv.at[h, i],
            device_id=sibling,
            device_id_type=MESH,
        )

    def project(h):
        proj[...] = dot(follow[...], ext[:, HALF * h : HALF * h + HALF]).astype(BF16)

    def terms(h, half):
        term = dot(rest[HALF * half : HALF * half + HALF, :], proj[...])
        for j in range(8):
            k = 8 * half + j
            rawa[R * k : R * k + R, :] = term[2 * R * j : 2 * R * j + R, :]
            own[1, h, k // 4, R * (k % 4) : R * (k % 4) + R, :] = term[
                2 * R * j + R : 2 * R * j + 2 * R, :
            ]

    def arrange(h):
        flipped = rawa[...].T
        for u in range(4):
            own[0, h, u] = flipped[Q * u : Q * u + Q, :]
        to_sibling(h, 0).start()
        to_sibling(h, 1).start()

    place1 = jnp.where(core == 0, x, y)
    place2 = jnp.where(core == 0, y, x)

    def on_ring(is_x, at):
        return device(jnp.where(is_x, y, at), z, jnp.where(is_x, at, x), core)

    data = own.at[core]
    ahead = ((place1 + 1) % 4, (place1 + 3) % 4)
    behind = ((place1 + 3) % 4, (place1 + 1) % 4)
    across = (place1 + 2) % 4
    def copy1(h, slot):
        if slot == 4:
            src, dst, to = data.at[h, behind[h]], ring1.at[h, 2], behind[h]
        else:
            chunk = across if slot < 2 else ahead[h]
            part = pl.ds(PART * (slot % 2), PART)
            src, dst, to = data.at[h, chunk, part], ring1.at[h, slot // 2, part], ahead[h]
        return pltpu.make_async_remote_copy(
            src_ref=src,
            dst_ref=dst,
            send_sem=r1_send.at[h, slot],
            recv_sem=r1_recv.at[h, slot],
            device_id=on_ring(core == 0, to),
            device_id_type=MESH,
        )

    def join(h):
        for i in range(2):
            part = pl.ds(PART * i, PART)
            to_sibling(h, i).wait()
            for u in range(4):
                data[h, u, part] = data[h, u, part] + sib[h, u, part]
            copy1(h, i).start()

    def pass_on(h):
        for i in range(2):
            part = pl.ds(PART * i, PART)
            copy1(h, i).wait()
            data[h, ahead[h], part] = data[h, ahead[h], part] + ring1[h, 0, part]
            copy1(h, 2 + i).start()

    def copy2(h, k):
        to = (place2 + k) % 4
        return pltpu.make_async_remote_copy(
            src_ref=acc2.at[h, to],
            dst_ref=ring2.at[h, k - 1],
            send_sem=r2_send.at[h, k - 1],
            recv_sem=r2_recv.at[h, k - 1],
            device_id=on_ring(core == 1, to),
            device_id_type=MESH,
        )

    def turn(h):
        for slot in (2, 3, 4):
            copy1(h, slot).wait()
        mid[0:Q, :] = data[h, place1] + ring1[h, 1] + ring1[h, 2]
        mid[Q:128, :] = jnp.zeros((128 - Q, HALF), F32)
        turned = mid[...].T
        for v in range(4):
            acc2[h, v] = turned[Q * v : Q * v + Q, :]
        for k in (2, 1, 3):
            copy2(h, k).start()

    me = z * 2 + core

    def spread(to, source):
        return pltpu.make_async_remote_copy(
            src_ref=fin.at[to],
            dst_ref=last.at[source],
            send_sem=last_send.at[to],
            recv_sem=last_recv.at[source],
            device_id=device(y, to // 2, x, to % 2),
            device_id_type=MESH,
        )

    front = iota((8, 128), 1) < 48

    def settle(h):
        for k in (1, 2, 3):
            copy2(h, k).wait()
        mid[0:Q, 0:128] = acc2[h, place2] + ring2[h, 0] + ring2[h, 1] + ring2[h, 2]
        got = mid[:, 0:128]
        got = jnp.where(core == 1, got.T, got)
        for k in range(4):
            one8, two8, three8 = (got[R * k + 8 * i : R * k + 8 * i + 8, :] for i in range(3))
            to0, to1 = 8 * h + 2 * k, 8 * h + 2 * k + 1
            fin[to0, 0:8, :] = jnp.where(front, one8, pltpu.roll(two8, 48, 1))
            fin[to0, 8:16, :] = three8
            fin[to1, 0:8, :] = jnp.where(front, pltpu.roll(one8, 80, 1), two8)
            fin[to1, 8:16, :] = pltpu.roll(three8, 80, 1)

        def start(k, carry):
            @pl.when(k != me)
            def _():
                spread(k, me).start()

            return carry

        lax.fori_loop(8 * h, 8 * h + 8, start, 0)

    project(0)
    terms(0, 0)
    terms(0, 1)
    arrange(0)
    project(1)
    terms(1, 0)
    join(0)
    copy1(0, 4).start()
    terms(1, 1)
    arrange(1)
    for copy in ex1:
        copy.wait()
    q0 = local0 + from_edges(*(recvx[0, d] for d in range(4)))
    p1 = q0 - p0
    w1 = p1 / precond
    local1 = matvec(w1)
    sendx[1] = canonical(local1)
    ex2 = exchange(sendx.at[1], recvx.at[1], 2)
    for copy in ex2:
        copy.start()

    join(1)
    pass_on(0)
    copy1(1, 4).start()
    pass_on(1)
    for copy in ex2:
        copy.wait()
    q1 = local1 + from_edges(*(recvx[1, d] for d in range(4)))
    p2 = q1 - p1
    w2 = p2 / precond
    local2 = matvec(w2)
    sendx[2] = canonical(local2)
    ex3 = exchange(sendx.at[2], recvx.at[2], 3)
    for copy in ex3:
        copy.start()

    products = (
        0.5 * w0 * p0,
        0.5 * w0 * p1,
        0.5 * w1 * p1,
        0.5 * w1 * p2,
        0.5 * w2 * p2,
        w2 * local2,
    )
    rows = jnp.zeros((8, 128), F32)
    for i, product in enumerate(products):
        rows = jnp.where(row == i, jnp.sum(product, axis=0, keepdims=True), rows)
    sums = jnp.sum(rows, axis=1, keepdims=True)
    mine = jnp.sum(jnp.where(iota((8, 128), 1) == row, sums, 0.0), axis=0, keepdims=True)
    ar_send[0] = mine

    def gather(stage, k):
        return pltpu.make_async_remote_copy(
            src_ref=ar_send.at[stage],
            dst_ref=(ar1, ar2)[stage].at[k],
            send_sem=(a1_send, a2_send)[stage].at[k],
            recv_sem=(a1_recv, a2_recv)[stage].at[k],
            device_id=(plane_peer, column_peer)[stage](k),
            device_id_type=MESH,
        )

    def gather_start(stage):
        for k in range(1, 16):
            gather(stage, k).start()

    def gather_sum(stage, start):
        for k in range(1, 16):
            gather(stage, k).wait()
        total = start
        for k in range(1, 16):
            total = total + (ar1, ar2)[stage][k]
        return total

    gather_start(0)

    turn(0)
    turn(1)
    total1 = gather_sum(0, ar_send[0])
    ar_send[1] = total1
    gather_start(1)
    settle(0)
    settle(1)
    last[me] = fin[me]

    moments = gather_sum(1, ar_send[1])
    lane = iota((1, 128), 1)
    g = [
        jnp.sum(jnp.where(lane == i, moments, 0.0), axis=1, keepdims=True) for i in range(6)
    ]
    g[5] = g[5] - g[4]

    def form(u, v, shift):
        total = None
        for i, ui in enumerate(u):
            for j, vj in enumerate(v):
                if ui is None or vj is None:
                    continue
                part = ui * vj * (g[i + j] + g[i + j + 1] if shift else g[i + j])
                total = part if total is None else total + part
        return total

    def plus(u, s, v):
        return [
            p if q is None else (s * q if p is None else p + s * q) for p, q in zip(u, v)
        ]

    one = jnp.ones((1, 1), F32)
    scaled = [one, None, None]
    direction = [one, None, None]
    amount = [None, None, None]
    norm = form(scaled, scaled, False)
    for step in range(3):
        size = norm / form(direction, direction, True)
        amount = plus(amount, size, direction)
        if step < 2:
            image = plus(direction, one, [None] + direction[:2])
            scaled = plus(scaled, -size, image)
            following = form(scaled, scaled, False)
            direction = plus(scaled, following / norm, direction)
            norm = following
    for copy in ex3:
        copy.wait()
    q2 = local2 + from_edges(*(recvx[2, d] for d in range(4)))
    sol[...] = amount[0] * w0 + amount[1] * w1 + amount[2] * w2
    res[...] = p0 - (amount[0] * q0 + amount[1] * q1 + amount[2] * q2)
    results = [
        pltpu.make_async_copy(src, dst, result_sem.at[i])
        for i, (src, dst) in enumerate(((sol, sol_out), (res, res_out), (coarse, coarse_out)))
    ]
    results[0].start()
    results[1].start()


    def finish(k, carry):
        @pl.when(k != me)
        def _():
            spread(k, k).wait()

        return carry

    lax.fori_loop(0, 16, finish, 0)
    for colour in range(2):
        rows_of = last[colour]
        for k in range(1, 8):
            rows_of = rows_of + last[2 * k + colour]
        for i, part in enumerate((rows_of[0:8], pltpu.roll(rows_of[0:8], 80, 1), rows_of[8:16])):
            coarse[R * colour + 8 * i : R * colour + 8 * i + 8, :] = part[:, 0:48]
    results[2].start()
    store.wait()
    for copy in results:
        copy.wait()


def store_outputs(
    sol, res, follow_in, coarse, sol_out, res_out, next_hbm, coarse_out, out_sem
):
    part = NB // 4
    rows = [pl.ds(part * i, part) for i in range(4)]
    back = [
        pltpu.make_async_copy(follow_in.at[rows[i]], next_hbm.at[0, 0, rows[i]], out_sem.at[i])
        for i in range(4)
    ]
    for copy in back:
        copy.start()
    for k in range(8):
        sol_out[0, 0:1, 128 * k : 128 * k + 128] = sol[k : k + 1, :]
        res_out[0, 0:1, 128 * k : 128 * k + 128] = res[k : k + 1, :]
    coarse_out[...] = coarse[...]
    for copy in back:
        copy.wait()


def per_device(
    schur, rhs_local, edge_perm, chol_interior, coupling, boundary_diag, restrict, extend
):
    any_ = pl.BlockSpec(memory_space=pl.ANY)
    vmem = pl.BlockSpec(memory_space=pltpu.VMEM)
    dma = pltpu.SemaphoreType.DMA
    out = pl.pallas_call(
        kernel,
        out_shape=(
            jax.ShapeDtypeStruct((8, 128), F32),
            jax.ShapeDtypeStruct((8, 128), F32),
            jax.ShapeDtypeStruct((NB, NB), BF16),
            jax.ShapeDtypeStruct((48, 48), F32),
        ),
        in_specs=[pl.BlockSpec(memory_space=pltpu.HBM)] * 8,
        out_specs=(any_,) * 4,
        scratch_shapes=[
            pltpu.SMEM((2, 4), jnp.int32),
            pltpu.VMEM((1, NB), F32),
            pltpu.VMEM((8, 128), F32),
            pltpu.VMEM((8, 128, 128), F32),
            pltpu.VMEM((NB, NB), F32),
            pltpu.VMEM((NI, NI), F32),
            pltpu.VMEM((NI, NB), BF16),
            pltpu.VMEM((MC, NB), BF16),
            pltpu.VMEM((NB, MC), BF16),
            pltpu.VMEM((NI, NI), F32),
            pltpu.VMEM((NI, NB), BF16),
            pltpu.VMEM((NB, NB), BF16),
            pltpu.VMEM((NB, HALF), BF16),
            pltpu.VMEM((HALF, HALF), F32),
            pltpu.VMEM((2, 2, 4, Q, HALF), F32),
            pltpu.VMEM((2, 4, Q, HALF), F32),
            pltpu.VMEM((2, 3, Q, HALF), F32),
            pltpu.VMEM((128, HALF), F32),
            pltpu.VMEM((2, 4, Q, 128), F32),
            pltpu.VMEM((2, 3, Q, 128), F32),
            pltpu.VMEM((16, 16, 128), F32),
            pltpu.VMEM((16, 16, 128), F32),
            pltpu.VMEM((2, 8, 128), F32),
            pltpu.VMEM((8, 128), F32),
            pltpu.VMEM((8, 128), F32),
            pltpu.VMEM((48, 48), F32),
            pltpu.VMEM((16, 128), F32),
            pltpu.VMEM((4, 16, 128), F32),
            pltpu.VMEM((3, 8, 128), F32),
            pltpu.VMEM((3, 4, 8, 128), F32),
            pltpu.VMEM((2, 1, 128), F32),
            pltpu.VMEM((16, 1, 128), F32),
            pltpu.VMEM((16, 1, 128), F32),
            dma((8,)),
            dma((8,)),
            dma,
            dma((3,)),
            dma((4, 4)),
            dma((4, 4)),
            dma((2, 2)),
            dma((2, 2)),
            dma((2, 5)),
            dma((2, 5)),
            dma((2, 3)),
            dma((2, 3)),
            dma((16,)),
            dma((16,)),
            dma((16,)),
            dma((16,)),
            dma((16,)),
            dma((16,)),
        ],
        compiler_params=pltpu.CompilerParams(
            collective_id=0, has_side_effects=True, vmem_limit_bytes=36 * 1024 * 1024
        ),
        name="interface_and_coarse",
    )(
        *(
            pltpu.with_memory_space_constraint(array, pltpu.HBM)
            for array in (
                edge_perm[0, 0].T,
                boundary_diag[0],
                rhs_local.reshape(8, 128),
                schur[0, 0],
                chol_interior[0, 0],
                coupling[0, 0],
                restrict[0, 0],
                extend[0, 0],
            )
        )
    )
    return pl.pallas_call(
        store_outputs,
        out_shape=(
            jax.ShapeDtypeStruct((1, 1, NB), F32),
            jax.ShapeDtypeStruct((1, 1, NB), F32),
            jax.ShapeDtypeStruct((1, 1, NB, NB), BF16),
            jax.ShapeDtypeStruct((48, 48), F32),
        ),
        in_specs=[vmem, vmem, any_, vmem],
        out_specs=(vmem, vmem, any_, vmem),
        scratch_shapes=[dma((4,))],
        compiler_params=pltpu.CompilerParams(vmem_limit_bytes=4 * 1024 * 1024),
        name="store_outputs",
    )(*out)


def solution(mesh):
    wide = P("sx", "sy", None, None)
    flat = P("sx", "sy", None)
    return jax.shard_map(
        per_device,
        mesh=mesh,
        in_specs=(wide, flat, wide, wide, wide, flat, wide, wide),
        out_specs=(flat, flat, wide, P("sx", "sy")),
        check_vma=False,
    )
```
